32 devices in a mesh: member: 2 (over x), band: 16 (over z, y, core).
Axes of the slice: x: 2, y: 2, z: 4, core: 2. Of those that a mesh axis runs over, the one named last changes fastest.
Arguments:
- grid_in: bfloat16 [32, 274, 5248], P(('member', 'band')), parts along dimension 0, may hold values from -6 to 6
- legendre: bfloat16 [16, 2, 640, 8], P('band'), may hold values from -2 to 2
- gauss_weight: float32 [8], replicated, may hold values from 0.2 to 2
- vertical_modes: float32 [137, 137], replicated
- coupling: float32 [137, 137], replicated, may hold values from -0.5 to 0.5
- mode_rates: float32 [137], replicated, may hold values from 0.1 to 10
- loop_length: int32 [16], replicated, may hold values from 20 to 5136, as said below
- lat_order: int32 [16], replicated, may hold values from 0 to 15, each once
- wave_number: int32 [16], replicated, may hold values from 0 to 1279, as said below
Outputs:
- grid_out: bfloat16 [32, 274, 5248], P(('member', 'band')), parts along dimension 0
The draws below stay inside these ranges and needn't reach their ends.
There are 2 independent parts, one for each index of `member`. The reference program is written for one: setup_inputs(seed, part) draws one part's arguments, and reference() takes and returns one part's arrays. A program takes and returns all parts, laid end to end along the dimension named above; an argument that names none is the same for every part. Nothing has to cross between parts.
Inputs may be any that keep to these rules, and one draw needn't show every extreme that they name: loop_length[t] = 20 + 4 k with k not falling from the poles toward the equator, equal for latitudes t and 15 - t; the equatorial loops have 5248 - 112 points. Row i of grid_in and grid_out holds latitude lat_order[i]. `wave_number`: distinct values.
All inputs are finite; a program needn't handle non-finite values.
Results may differ from the reference program's by a relative error of at most 0.013.
Values may be sent and summed in bfloat16 or wider, within the bound.
A program may use at most 64 MiB of HBM per device.

```python
import math
import jax
import jax.numpy as jnp
from jax import lax

TRUNC = 1279
LOOP_PAD = 5248
LEV = 137
NLAT = 16
NLAT_H = 8
M_WIN = 16
FL = 274
NHALF = 640


def draw_vertical_modes(key, part):
    gaussian = jax.random.normal(key, (LEV, LEV), jnp.float32)
    basis, upper_part = jnp.linalg.qr(gaussian)
    return basis.astype(jnp.float32)


def draw_loop_length(key, part):
    top_index = (LOOP_PAD - 132) // 4
    loop_key = jax.random.fold_in(key, 7)
    picked = jax.random.randint(loop_key, (NLAT_H,), 0, top_index + 1, dtype=jnp.int32)
    loop_index = jnp.sort(picked)
    loop_index = loop_index.at[NLAT_H - 1].set(top_index)
    north_len = 20 + 4 * loop_index
    return jnp.concatenate([north_len, north_len[::-1]]).astype(jnp.int32)


def draw_wave_number(key, part):
    first_key = jax.random.fold_in(key, 11)
    second_key = jax.random.fold_in(key, 23)
    chosen = jax.random.permutation(first_key, TRUNC + 1)[:M_WIN].astype(jnp.int32)
    has_top = jnp.any(chosen == TRUNC)
    chosen = chosen.at[0].set(jnp.where(has_top, chosen[0], TRUNC))
    has_zero = jnp.any(chosen == 0)
    place = jnp.where(chosen[1] == TRUNC, 2, 1)
    chosen = chosen.at[place].set(jnp.where(has_zero, chosen[place], 0))
    shuffle = jax.random.permutation(second_key, M_WIN)
    return chosen[shuffle].astype(jnp.int32)


def steps_of(stream_key, extent, pieces, smallest, high):
    def one(axis_at, blocks):
        heights = jax.random.uniform(jax.random.fold_in(jax.random.fold_in(stream_key, 6), axis_at), (blocks,), jnp.float32, smallest / len(pieces), high / len(pieces))
        return jnp.repeat(jnp.exp(heights), extent[axis_at] // blocks).reshape((-1,) + (1,) * (len(extent) - axis_at - 1))

    level = one(*pieces[0])
    for cut in pieces[1:]:
        level = level * one(*cut)
    return level


def noise(stream_key, dims, width, reach, cuts=(), kind=jnp.bfloat16):
    gain = steps_of(stream_key, dims, cuts, -0.22, 0.18) if cuts else 1.0
    entries = jax.random.normal(stream_key, dims, jnp.float32) * width * gain
    return jnp.minimum(jnp.maximum(entries, -reach), reach).astype(kind)


def setup_inputs(seed: int = 0, part: int = 0) -> dict:
    key_of = jax.random.split(jax.random.key(seed), 10)
    part_splits = jax.random.split(jax.random.fold_in(key_of[9], part), 10)
    grid_in = noise(part_splits[0], (NLAT, FL, LOOP_PAD), 1.0, 6.0, ((0, 16),))
    legendre = noise(key_of[1], (M_WIN, 2, NHALF, NLAT_H), NLAT_H ** -0.5, 2.0, ((0, 16),))
    gauss_weight = jnp.clip(jnp.exp(jax.random.uniform(key_of[2], (NLAT_H,), jnp.float32, math.log(0.2), math.log(2.0))), 0.2, 2.0)
    vertical_modes = draw_vertical_modes(jax.random.fold_in(key_of[9], 71), part)
    coupling = noise(key_of[4], (LEV, LEV), LEV ** -0.5, 0.5, (), jnp.float32)
    mode_rates = jnp.clip(jnp.exp(jax.random.uniform(key_of[5], (LEV,), jnp.float32, math.log(0.1), math.log(10.0))), 0.1, 10.0)
    loop_length = draw_loop_length(jax.random.fold_in(key_of[9], 71), part)
    lat_order = jax.random.permutation(key_of[7], NLAT).astype(jnp.int32)
    wave_number = draw_wave_number(jax.random.fold_in(key_of[9], 71), part)
    return {"grid_in": grid_in, "legendre": legendre, "gauss_weight": gauss_weight, "vertical_modes": vertical_modes, "coupling": coupling, "mode_rates": mode_rates, "loop_length": loop_length, "lat_order": lat_order, "wave_number": wave_number}


implicit_step = 0.5
highest = lax.Precision.HIGHEST

def loop_tables(length, wave_list, block_count):
    offsets = jnp.arange(128, dtype=jnp.int32)
    inner_turn = offsets[:, None] * wave_list[None, :] % length
    angles = inner_turn.astype(jnp.float32) * (2.0 * math.pi) / length.astype(jnp.float32)
    inner_table = jnp.concatenate([jnp.cos(angles), jnp.sin(angles)], axis=1).astype(jnp.bfloat16)
    block_index = jnp.arange(block_count, dtype=jnp.int32)
    outer_turn = block_index[:, None] * 128 * wave_list[None, :] % length
    phases = outer_turn.astype(jnp.float32) * (2.0 * math.pi) / length.astype(jnp.float32)
    return (inner_table, jnp.cos(phases), jnp.sin(phases))

def forward_loop(one_loop, length, wave_list):
    field_count, loop_width = one_loop.shape
    block_count = loop_width // 128
    wave_count = wave_list.shape[0]
    inner_table, cos_turn, sin_turn = loop_tables(length, wave_list, block_count)
    inside = jnp.arange(loop_width, dtype=jnp.int32) < length
    masked = jnp.where(inside[None, :], one_loop, jnp.zeros((), one_loop.dtype))
    products = jnp.dot(masked.reshape(field_count * block_count, 128).astype(jnp.float32), inner_table.astype(jnp.float32), preferred_element_type=jnp.float32)
    products = products.reshape(field_count, block_count, 2, wave_count)
    real_part = jnp.sum(cos_turn * products[:, :, 0] - sin_turn * products[:, :, 1], axis=1)
    imag_part = -jnp.sum(sin_turn * products[:, :, 0] + cos_turn * products[:, :, 1], axis=1)
    inverse_len = 1.0 / length.astype(jnp.float32)
    together = jnp.concatenate([real_part, imag_part], axis=0) * inverse_len
    resolved = 2 * wave_list < length
    together = jnp.where(resolved[None, :], together, 0.0)
    return together.T.astype(jnp.bfloat16)

def inverse_loop(fourier, length, wave_list, loop_width):
    block_count = loop_width // 128
    wave_count = wave_list.shape[0]
    field_count = fourier.shape[1] // 2
    inner_table, cos_turn, sin_turn = loop_tables(length, wave_list, block_count)
    doubling = jnp.where(wave_list == 0, 1.0, 2.0).astype(jnp.float32)
    real_part = fourier[:, :field_count].astype(jnp.float32).T * doubling
    imag_part = fourier[:, field_count:].astype(jnp.float32).T * doubling
    cosine_part = real_part[:, None, :] * cos_turn[None] - imag_part[:, None, :] * sin_turn[None]
    sine_part = -(real_part[:, None, :] * sin_turn[None] + imag_part[:, None, :] * cos_turn[None])
    combined = jnp.concatenate([cosine_part, sine_part], axis=2).astype(jnp.bfloat16)
    points = lax.dot_general(combined.reshape(field_count * block_count, 2 * wave_count).astype(jnp.float32), inner_table.astype(jnp.float32), (((1,), (1,)), ((), ())), preferred_element_type=jnp.float32)
    points = points.reshape(field_count, loop_width)
    inside = jnp.arange(loop_width, dtype=jnp.int32) < length
    return jnp.where(inside[None, :], points, 0.0).astype(jnp.bfloat16)

def semi_implicit(spectral, wave_values, vertical_modes, coupling, mode_rates):
    half_rows = spectral.shape[-2]
    level_count = vertical_modes.shape[0]
    parity = jnp.arange(2, dtype=jnp.int32)
    row_index = jnp.arange(half_rows, dtype=jnp.int32)
    degree = wave_values[..., None, None] + parity[:, None] + 2 * row_index[None, :]
    kept_rows = degree <= TRUNC
    spectral = jnp.where(kept_rows[..., None], spectral, 0.0)
    damping = (degree * (degree + 1)).astype(jnp.float32) / float(TRUNC * (TRUNC + 1))
    reshaped = spectral.reshape(spectral.shape[:-1] + (2, 2, level_count))
    divergence = reshaped[..., 0, :]
    pressure = reshaped[..., 1, :]
    factor_e = damping[..., None, None]
    right_side = divergence - implicit_step * factor_e * jnp.einsum('...l,kl->...k', pressure, coupling, precision=highest)
    in_modes = jnp.einsum('...l,lk->...k', right_side, vertical_modes, precision=highest)
    in_modes = in_modes / (1.0 + implicit_step * factor_e * mode_rates)
    new_div = jnp.einsum('...k,lk->...l', in_modes, vertical_modes, precision=highest)
    new_press = pressure - implicit_step * jnp.einsum('...l,kl->...k', new_div, coupling, precision=highest)
    updated = jnp.stack([new_div, new_press], axis=-2)
    return updated.reshape(spectral.shape).astype(jnp.bfloat16)

def reference(grid_in, legendre, gauss_weight, vertical_modes, coupling, mode_rates, loop_length, lat_order, wave_number):
    lat_count, field_count, loop_width = grid_in.shape
    half_count = lat_count // 2
    row_lengths = jnp.take(loop_length, lat_order)

    def forward_one(scan_item):
        return forward_loop(scan_item[0], scan_item[1], wave_number)
    fourier = lax.map(forward_one, (grid_in, row_lengths))
    row_of_lat = jnp.argsort(lat_order)
    northern = jnp.take(fourier, row_of_lat[:half_count], axis=0).astype(jnp.float32)
    southern = jnp.take(fourier, row_of_lat[::-1][:half_count], axis=0).astype(jnp.float32)
    weight = gauss_weight[:, None, None]
    even_part = (weight * (northern + southern)).astype(jnp.bfloat16)
    odd_part = (weight * (northern - southern)).astype(jnp.bfloat16)
    stacked = jnp.stack([even_part, odd_part], axis=0)
    per_wave = jnp.transpose(stacked, (2, 0, 1, 3))

    def wave_one(scan_item):
        table_block, columns, wave_value = scan_item
        table_wide = table_block.astype(jnp.float32)
        spectral = jnp.einsum('prj,pjc->prc', table_wide, columns.astype(jnp.float32), precision=highest)
        updated = semi_implicit(spectral, wave_value, vertical_modes, coupling, mode_rates)
        summed = jnp.einsum('prj,prc->pjc', table_wide, updated.astype(jnp.float32), precision=highest)
        northern_back = summed[0] + summed[1]
        southern_back = summed[0] - summed[1]
        by_lat = jnp.concatenate([northern_back, southern_back[::-1]], axis=0)
        resolved = 2 * wave_value < loop_length
        return jnp.where(resolved[:, None], by_lat, 0.0).astype(jnp.bfloat16)
    back_waves = lax.map(wave_one, (legendre, per_wave, wave_number))
    by_rows = jnp.take(back_waves, lat_order, axis=1)
    per_row = jnp.transpose(by_rows, (1, 0, 2))

    def inverse_one(scan_item):
        return inverse_loop(scan_item[0], scan_item[1], wave_number, loop_width)
    return lax.map(inverse_one, (per_row, row_lengths))
```

```python
import functools
import math

import jax
import jax.numpy as jnp
from jax import lax
from jax.experimental import pallas as pl
from jax.experimental.pallas import tpu as pltpu
from jax.sharding import PartitionSpec as P

TRUNC = 1279
STEP = 0.5
F32 = jnp.float32
BF16 = jnp.bfloat16
HIGHEST = lax.Precision.HIGHEST
NT = (((1,), (1,)), ((), ()))
NN = (((1,), (0,)), ((), ()))
TN = (((0,), (0,)), ((), ()))


def dot(a, b, dims=NN, precision=None):
    return lax.dot_general(a, b, dims, precision=precision, preferred_element_type=F32)


def iota(shape, dim):
    return lax.broadcasted_iota(jnp.int32, shape, dim)


def sin_cos(turns, quarter_shift):
    quarter = jnp.floor(4.0 * turns + 0.5)
    y = (turns - 0.25 * quarter) * (2.0 * math.pi)
    z = y * y
    sine = y + y * z * (-1.6666654611e-1 + z * (8.3321608736e-3 + z * (-1.9515295891e-4)))
    cosine = 1.0 - 0.5 * z + z * z * (4.166664568298827e-2 + z * (-1.388731625493765e-3 + z * 2.443315711809948e-5))
    k = quarter.astype(jnp.int32) - quarter_shift
    swap = (k & 1) == 1
    cos_sign = jnp.where(((k + 1) & 2) == 0, 1.0, -1.0)
    sin_sign = jnp.where((k & 2) == 0, 1.0, -1.0)
    return (
        cos_sign * jnp.where(swap, sine, cosine),
        sin_sign * jnp.where(swap, cosine, sine),
    )


def spread(values, index, start):
    out = jnp.full(index.shape, start, F32)
    for at, value in enumerate(values):
        out = jnp.where(index == at, value, out)
    return out


def chunk_bounds(blocks, pieces):
    edges = [blocks * i // pieces for i in range(pieces + 1)]
    return [(a * 128, b * 128) for a, b in zip(edges[:-1], edges[1:]) if b > a]


def main_kernel(
    groups,
    chunks,
    grid_hbm,
    leg_ref,
    gauss_ref,
    modes_ref,
    coupling_ref,
    rates_ref,
    length_ref,
    order_ref,
    wave_ref,
    coef_ref,
    table_ref,
    grid_vmem,
    wf_ref,
    wb_ref,
    mu_ref,
    send_one,
    recv_one,
    send_two,
    recv_two,
    in_sem,
    ssem_one,
    rsem_one,
    ssem_two,
    rsem_two,
):
    me = lax.axis_index("band")
    field_count, width = grid_vmem.shape
    levels = modes_ref.shape[0]
    half_rows, nh = leg_ref.shape[2], leg_ref.shape[3]
    lats = order_ref.shape[0]
    rows = 2 * groups
    kpad = wb_ref.shape[1]

    loads = []
    for at, (lo, hi) in enumerate(chunks):
        copy = pltpu.make_async_copy(
            grid_hbm.at[0, :, lo:hi], grid_vmem.at[:, lo:hi], in_sem.at[at]
        )
        copy.start()
        loads.append(copy)

    barrier = pltpu.get_barrier_semaphore()

    def each_peer(body):
        if groups <= 16:
            for step in range(1, groups):
                body(lax.rem(me + step, groups))
        else:

            def step_body(step, carry):
                body(lax.rem(me + step, groups))
                return carry

            lax.fori_loop(1, groups, step_body, 0)

    each_peer(lambda peer: pl.semaphore_signal(barrier, inc=1, device_id={"band": peer}))

    length = length_ref[order_ref[me]]
    length_f = length.astype(F32)
    row_id = iota((rows, 128), 0)
    lane_id = iota((rows, 128), 1)
    row_q = row_id & 1
    wave_rows = spread([wave_ref[d].astype(F32) for d in range(groups)], row_id >> 1, 0.0)
    inverse_len = 1.0 / jnp.full((rows, 128), length_f, F32)

    def turns_of(product):
        return (product - jnp.floor(product * inverse_len + 0.5) * length_f) * inverse_len

    inner_c, inner_s = sin_cos(turns_of(wave_rows * lane_id.astype(F32)), row_q)
    outer_c, outer_s = sin_cos(turns_of(wave_rows * (lane_id * 128).astype(F32)), 0)
    scale = jnp.where(2.0 * wave_rows < length_f, inverse_len, 0.0)
    scale = jnp.where(row_q == 0, scale, -scale)[:, :1]
    for a in range(width // 128):
        block = outer_c[:, a : a + 1] * inner_c - outer_s[:, a : a + 1] * inner_s
        block = jnp.where(lane_id < length - 128 * a, block, 0.0)
        table_ref[:, a * 128 : (a + 1) * 128] = block.astype(BF16)

    total = jnp.zeros((rows, field_count), F32)
    for copy, (lo, hi) in zip(loads, chunks):
        copy.wait()
        total += dot(table_ref[:, lo:hi], grid_vmem[:, lo:hi], NT)
    fourier = total * scale

    def exchange(values, send, recv, ssem, rsem):
        packed = values.astype(BF16)
        for d in range(groups):
            send[d] = packed[2 * d : 2 * d + 2, :]

        def start(peer):
            pltpu.make_async_remote_copy(
                src_ref=send.at[peer],
                dst_ref=recv.at[me],
                send_sem=ssem.at[peer],
                recv_sem=rsem.at[me],
                device_id={"band": peer},
            ).start()

        def finish(peer):
            copy = pltpu.make_async_remote_copy(
                src_ref=send.at[peer],
                dst_ref=recv.at[peer],
                send_sem=ssem.at[peer],
                recv_sem=rsem.at[peer],
                device_id={"band": peer},
            )
            copy.wait_recv()
            copy.wait_send()

        return start, finish

    start, finish = exchange(fourier, send_one, recv_one, ssem_one, rsem_one)
    pl.semaphore_wait(barrier, groups - 1)
    each_peer(start)
    recv_one[me] = send_one[me]

    modes = modes_ref[...]
    coupling = coupling_ref[...]
    wf_ref[...] = jnp.zeros(wf_ref.shape, F32)
    wb_ref[...] = jnp.zeros(wb_ref.shape, F32)
    mu_ref[...] = jnp.zeros(mu_ref.shape, F32)
    mu_ref[:, 0:levels] = rates_ref[...].reshape(1, levels)
    wf_ref[0:levels, 0:levels] = modes
    wf_ref[levels : 2 * levels, kpad : kpad + levels] = dot(coupling, modes, TN, HIGHEST)
    wb_ref[0:levels, 0:levels] = modes
    wb_ref[levels : 2 * levels, 0:levels] = -STEP * dot(coupling, modes, NN, HIGHEST)
    wf = wf_ref[...].astype(BF16)
    wb = wb_ref[...].astype(BF16)

    wave = wave_ref[me]
    order = [order_ref[i] for i in range(lats)]
    order_f = [o.astype(F32) for o in order]
    gauss = [gauss_ref[jnp.minimum(o, lats - 1 - o)] for o in order]
    solved = [jnp.where(2 * wave < length_ref[o], 1.0, 0.0) for o in order]
    boost = jnp.where(wave == 0, 1.0, 2.0)

    lane_one = iota((1, 2 * rows), 1)
    lane_row = jnp.where(lane_one < rows, lane_one, lane_one - rows)
    lane_lat = spread(order_f, lane_row >> 1, 0.0)
    lane_gauss = spread(gauss, lane_row >> 1, 0.0)
    north_j = iota((nh, 2 * rows), 0).astype(F32)
    col_row = iota((rows, nh), 0)
    col_lat = spread(order_f, col_row >> 1, 0.0)
    col_scale = spread(solved, iota((rows, 1), 0) >> 1, 0.0) * boost
    col_scale = jnp.where((iota((rows, 1), 0) & 1) == 0, col_scale, -col_scale)
    col_j = iota((rows, nh), 1).astype(F32)

    denom = float(TRUNC * (TRUNC + 1))
    m_parts, lt_parts, g_parts = [], [], []
    for p in range(2):
        leg = leg_ref[0, p]
        degree = wave + p + 2 * iota((half_rows, 1), 0)
        damp = (degree * (degree + 1)).astype(F32) * (STEP / denom)
        degree_lane = wave + p + 2 * iota((1, half_rows), 1)
        kept = jnp.where(degree_lane <= TRUNC, 1.0, 0.0)
        g_parts.append(1.0 / (1.0 + damp * mu_ref[...]))
        sign = 1.0 if p == 0 else -1.0
        pick_lane = jnp.where(lane_lat == north_j, 1.0, 0.0) + jnp.where(
            lane_lat == (lats - 1) - north_j, sign, 0.0
        )
        pick_col = jnp.where(col_lat == col_j, 1.0, 0.0) + jnp.where(
            col_lat == (lats - 1) - col_j, sign, 0.0
        )
        weight = jnp.where(lane_one < rows, 1.0, -damp) * lane_gauss
        for q in range(2):
            chosen = jnp.where((lane_one & 1) == q, pick_lane, 0.0).astype(BF16)
            m_parts.append((dot(leg, chosen) * weight).astype(BF16))
            chosen = jnp.where((col_row & 1) == q, pick_col, 0.0).astype(BF16)
            lt_parts.append((dot(chosen, leg, NT) * kept * col_scale).astype(BF16))
    through = sum(dot(lt, m) for lt, m in zip(lt_parts, m_parts))[:, 0:rows].astype(BF16)

    each_peer(finish)
    arrived = recv_one[...].reshape(rows, field_count)
    in_modes = dot(arrived, wf).astype(BF16)
    stacked = jnp.concatenate([in_modes[:, :kpad], in_modes[:, kpad:]], axis=0)
    passed = dot(through, arrived)
    back = jnp.zeros((rows, kpad), F32)
    for at in range(4):
        solved_part = (dot(m_parts[at], stacked) * g_parts[at // 2]).astype(BF16)
        back += dot(lt_parts[at], solved_part)
    result = dot(back.astype(BF16), wb, NT)
    result += jnp.where(iota((rows, field_count), 1) >= levels, passed, 0.0)

    start, finish = exchange(result, send_two, recv_two, ssem_two, rsem_two)
    each_peer(start)
    recv_two[me] = send_two[me]
    each_peer(finish)
    coef_ref[...] = recv_two[...].reshape(rows, field_count)


def inverse_kernel(coef_ref, table_ref, out_ref):
    out_ref[0] = dot(coef_ref[...], table_ref[...], TN).astype(BF16)


def per_device(
    groups,
    grid_in,
    legendre,
    gauss_weight,
    vertical_modes,
    coupling,
    mode_rates,
    loop_length,
    lat_order,
    wave_number,
):
    loop_count, field_count, width = grid_in.shape
    assert loop_count == 1 and legendre.shape[0] == 1
    rows = 2 * groups
    levels = vertical_modes.shape[0]
    kpad = -(-levels // 128) * 128
    chunks = chunk_bounds(width // 128, 8)
    vmem = pl.BlockSpec(memory_space=pltpu.VMEM)
    smem = pl.BlockSpec(memory_space=pltpu.SMEM)
    slot = pltpu.VMEM((groups, 2, field_count), BF16)
    sems = pltpu.SemaphoreType.DMA((groups,))
    coef, table = pl.pallas_call(
        functools.partial(main_kernel, groups, chunks),
        out_shape=(
            jax.ShapeDtypeStruct((rows, field_count), BF16),
            jax.ShapeDtypeStruct((rows, width), BF16),
        ),
        in_specs=[pl.BlockSpec(memory_space=pl.ANY), vmem, smem, vmem, vmem, vmem, smem, smem, smem],
        out_specs=(vmem, vmem),
        scratch_shapes=[
            pltpu.VMEM((field_count, width), BF16),
            pltpu.VMEM((2 * levels, 2 * kpad), F32),
            pltpu.VMEM((2 * levels, kpad), F32),
            pltpu.VMEM((1, kpad), F32),
            slot,
            slot,
            slot,
            slot,
            pltpu.SemaphoreType.DMA((len(chunks),)),
            sems,
            sems,
            sems,
            sems,
        ],
        compiler_params=pltpu.CompilerParams(
            collective_id=0, has_side_effects=True, vmem_limit_bytes=32 * 1024 * 1024
        ),
        name="forward_spectral",
    )(
        grid_in,
        legendre,
        gauss_weight,
        vertical_modes,
        coupling,
        mode_rates,
        loop_length,
        lat_order,
        wave_number,
    )
    tile = 640
    return pl.pallas_call(
        inverse_kernel,
        grid=(-(-width // tile),),
        out_shape=jax.ShapeDtypeStruct(grid_in.shape, BF16),
        in_specs=[
            pl.BlockSpec((rows, field_count), lambda i: (0, 0)),
            pl.BlockSpec((rows, tile), lambda i: (0, i)),
        ],
        out_specs=pl.BlockSpec((1, field_count, tile), lambda i: (0, 0, i)),
        compiler_params=pltpu.CompilerParams(vmem_limit_bytes=32 * 1024 * 1024),
        name="inverse",
    )(coef, table)


def solution(mesh):
    groups = mesh.shape["band"]
    placed = (
        P(("member", "band"), None, None),
        P("band", None, None, None),
        P(),
        P(),
        P(),
        P(),
        P(),
        P(),
        P(),
    )
    return jax.shard_map(
        functools.partial(per_device, groups),
        mesh=mesh,
        in_specs=placed,
        out_specs=P(("member", "band"), None, None),
        check_vma=False,
    )
```

```python
import functools
import math

import jax
import jax.numpy as jnp
from jax import lax
from jax.experimental import pallas as pl
from jax.experimental.pallas import tpu as pltpu
from jax.sharding import PartitionSpec as P

TRUNC = 1279
STEP = 0.5
F32 = jnp.float32
BF16 = jnp.bfloat16
HIGHEST = lax.Precision.HIGHEST
NT = (((1,), (1,)), ((), ()))
NN = (((1,), (0,)), ((), ()))
TN = (((0,), (0,)), ((), ()))


def dot(a, b, dims=NN, precision=None):
    return lax.dot_general(a, b, dims, precision=precision, preferred_element_type=F32)


def iota(shape, dim):
    return lax.broadcasted_iota(jnp.int32, shape, dim)


def sin_cos(turns, quarter_shift):
    quarter = jnp.floor(4.0 * turns + 0.5)
    y = (turns - 0.25 * quarter) * (2.0 * math.pi)
    z = y * y
    sine = y + y * z * (-1.6666654611e-1 + z * (8.3321608736e-3 + z * (-1.9515295891e-4)))
    cosine = 1.0 - 0.5 * z + z * z * (4.166664568298827e-2 + z * (-1.388731625493765e-3 + z * 2.443315711809948e-5))
    k = quarter.astype(jnp.int32) - quarter_shift
    swap = (k & 1) == 1
    cos_sign = jnp.where(((k + 1) & 2) == 0, 1.0, -1.0)
    sin_sign = jnp.where((k & 2) == 0, 1.0, -1.0)
    return (
        cos_sign * jnp.where(swap, sine, cosine),
        sin_sign * jnp.where(swap, cosine, sine),
    )


def spread(values, index, start):
    out = jnp.full(index.shape, start, F32)
    for at, value in enumerate(values):
        out = jnp.where(index == at, value, out)
    return out


def chunk_bounds(blocks, pieces):
    edges = [blocks * i // pieces for i in range(pieces + 1)]
    return [(a * 128, b * 128) for a, b in zip(edges[:-1], edges[1:]) if b > a]


def main_kernel(
    groups,
    chunks,
    grid_hbm,
    leg_hbm,
    gauss_hbm,
    modes_hbm,
    coupling_hbm,
    rates_hbm,
    length_hbm,
    order_hbm,
    wave_hbm,
    coef_ref,
    table_ref,
    grid_vmem,
    leg_ref,
    gauss_ref,
    modes_ref,
    coupling_ref,
    rates_ref,
    length_ref,
    order_ref,
    wave_ref,
    wf_ref,
    wb_ref,
    mu_ref,
    send_one,
    recv_one,
    send_two,
    recv_two,
    in_sem,
    small_sem,
    ssem_one,
    rsem_one,
    ssem_two,
    rsem_two,
):
    me = lax.axis_index("band")
    field_count, width = grid_vmem.shape
    levels = modes_ref.shape[0]
    nh, half_rows = leg_ref.shape[2], leg_ref.shape[3]
    lats = order_ref.shape[0]
    rows = 2 * groups
    kpad = wb_ref.shape[1]

    scalars = []
    smalls = []
    for at, (source, target) in enumerate(
        (
            (order_hbm, order_ref),
            (length_hbm, length_ref),
            (wave_hbm, wave_ref),
            (gauss_hbm, gauss_ref),
            (leg_hbm, leg_ref),
            (modes_hbm, modes_ref),
            (coupling_hbm, coupling_ref),
            (rates_hbm, rates_ref),
        )
    ):
        copy = pltpu.make_async_copy(source, target, small_sem.at[at])
        copy.start()
        (scalars if at < 4 else smalls).append(copy)
    loads = []
    for at, (lo, hi) in enumerate(chunks):
        copy = pltpu.make_async_copy(
            grid_hbm.at[0, :, lo:hi], grid_vmem.at[:, lo:hi], in_sem.at[at]
        )
        copy.start()
        loads.append(copy)

    barrier = pltpu.get_barrier_semaphore()

    def each_peer(body):
        if groups <= 16:
            for step in range(1, groups):
                body(lax.rem(me + step, groups))
        else:

            def step_body(step, carry):
                body(lax.rem(me + step, groups))
                return carry

            lax.fori_loop(1, groups, step_body, 0)

    each_peer(lambda peer: pl.semaphore_signal(barrier, inc=1, device_id={"band": peer}))

    for copy in scalars:
        copy.wait()

    length = length_ref[order_ref[me]]
    length_f = length.astype(F32)
    row_id = iota((rows, 128), 0)
    lane_id = iota((rows, 128), 1)
    row_q = row_id & 1
    wave_rows = spread([wave_ref[d].astype(F32) for d in range(groups)], row_id >> 1, 0.0)
    inverse_len = 1.0 / jnp.full((rows, 128), length_f, F32)

    def turns_of(product):
        return (product - jnp.floor(product * inverse_len + 0.5) * length_f) * inverse_len

    inner_c, inner_s = sin_cos(turns_of(wave_rows * lane_id.astype(F32)), row_q)
    outer_c, outer_s = sin_cos(turns_of(wave_rows * (lane_id * 128).astype(F32)), 0)
    scale = jnp.where(2.0 * wave_rows < length_f, inverse_len, 0.0)
    scale = jnp.where(row_q == 0, scale, -scale)[:, :1]
    for a in range(width // 128):
        block = outer_c[:, a : a + 1] * inner_c - outer_s[:, a : a + 1] * inner_s
        block = jnp.where(lane_id < length - 128 * a, block, 0.0)
        table_ref[:, a * 128 : (a + 1) * 128] = block.astype(BF16)

    total = jnp.zeros((rows, field_count), F32)
    for copy, (lo, hi) in zip(loads, chunks):
        copy.wait()
        total += dot(table_ref[:, lo:hi], grid_vmem[:, lo:hi], NT)
    fourier = total * scale

    def exchange(values, send, recv, ssem, rsem):
        packed = values.astype(BF16)
        for d in range(groups):
            send[d] = packed[2 * d : 2 * d + 2, :]

        def start(peer):
            pltpu.make_async_remote_copy(
                src_ref=send.at[peer],
                dst_ref=recv.at[me],
                send_sem=ssem.at[peer],
                recv_sem=rsem.at[me],
                device_id={"band": peer},
            ).start()

        def finish(peer):
            copy = pltpu.make_async_remote_copy(
                src_ref=send.at[peer],
                dst_ref=recv.at[peer],
                send_sem=ssem.at[peer],
                recv_sem=rsem.at[peer],
                device_id={"band": peer},
            )
            copy.wait_recv()
            copy.wait_send()

        return start, finish

    start, finish = exchange(fourier, send_one, recv_one, ssem_one, rsem_one)
    pl.semaphore_wait(barrier, groups - 1)
    each_peer(start)
    recv_one[me] = send_one[me]

    for copy in smalls:
        copy.wait()
    modes = modes_ref[...]
    coupling = coupling_ref[...]
    wf_ref[...] = jnp.zeros(wf_ref.shape, F32)
    wb_ref[...] = jnp.zeros(wb_ref.shape, F32)
    mu_ref[...] = jnp.zeros(mu_ref.shape, F32)
    mu_ref[:, 0:levels] = rates_ref[...].reshape(1, levels)
    wf_ref[0:levels, 0:levels] = modes
    wf_ref[levels : 2 * levels, kpad : kpad + levels] = dot(coupling, modes, TN, HIGHEST)
    wb_ref[0:levels, 0:levels] = modes
    wb_ref[levels : 2 * levels, 0:levels] = -STEP * dot(coupling, modes, NN, HIGHEST)
    wf = wf_ref[...].astype(BF16)
    wb = wb_ref[...].astype(BF16)

    wave = wave_ref[me]
    order = [order_ref[i] for i in range(lats)]
    order_f = [o.astype(F32) for o in order]
    gauss = [gauss_ref[jnp.minimum(o, lats - 1 - o)] for o in order]
    solved = [jnp.where(2 * wave < length_ref[o], 1.0, 0.0) for o in order]
    boost = jnp.where(wave == 0, 1.0, 2.0)

    lane_one = iota((1, 2 * rows), 1)
    lane_row = jnp.where(lane_one < rows, lane_one, lane_one - rows)
    lane_lat = spread(order_f, lane_row >> 1, 0.0)
    lane_gauss = spread(gauss, lane_row >> 1, 0.0)
    north_j = iota((nh, 2 * rows), 0).astype(F32)
    col_row = iota((rows, nh), 0)
    col_lat = spread(order_f, col_row >> 1, 0.0)
    col_scale = spread(solved, iota((rows, 1), 0) >> 1, 0.0) * boost
    col_scale = jnp.where((iota((rows, 1), 0) & 1) == 0, col_scale, -col_scale)
    col_j = iota((rows, nh), 1).astype(F32)

    denom = float(TRUNC * (TRUNC + 1))
    m_parts, lt_parts, g_parts = [], [], []
    for p in range(2):
        leg = leg_ref[0, p]
        degree = wave + p + 2 * iota((half_rows, 1), 0)
        damp = (degree * (degree + 1)).astype(F32) * (STEP / denom)
        degree_lane = wave + p + 2 * iota((1, half_rows), 1)
        kept = jnp.where(degree_lane <= TRUNC, 1.0, 0.0)
        g_parts.append(1.0 / (1.0 + damp * mu_ref[...]))
        sign = 1.0 if p == 0 else -1.0
        pick_lane = jnp.where(lane_lat == north_j, 1.0, 0.0) + jnp.where(
            lane_lat == (lats - 1) - north_j, sign, 0.0
        )
        pick_col = jnp.where(col_lat == col_j, 1.0, 0.0) + jnp.where(
            col_lat == (lats - 1) - col_j, sign, 0.0
        )
        weight = jnp.where(lane_one < rows, 1.0, -damp) * lane_gauss
        for q in range(2):
            chosen = jnp.where((lane_one & 1) == q, pick_lane, 0.0).astype(BF16)
            m_parts.append((dot(leg, chosen, TN) * weight).astype(BF16))
            chosen = jnp.where((col_row & 1) == q, pick_col, 0.0).astype(BF16)
            lt_parts.append((dot(chosen, leg) * kept * col_scale).astype(BF16))
    through = sum(dot(lt, m) for lt, m in zip(lt_parts, m_parts))[:, 0:rows].astype(BF16)

    each_peer(finish)
    arrived = recv_one[...].reshape(rows, field_count)
    in_modes = dot(arrived, wf).astype(BF16)
    stacked = jnp.concatenate([in_modes[:, :kpad], in_modes[:, kpad:]], axis=0)
    passed = dot(through, arrived)
    back = jnp.zeros((rows, kpad), F32)
    for at in range(4):
        solved_part = (dot(m_parts[at], stacked) * g_parts[at // 2]).astype(BF16)
        back += dot(lt_parts[at], solved_part)
    result = dot(back.astype(BF16), wb, NT)
    result += jnp.where(iota((rows, field_count), 1) >= levels, passed, 0.0)

    start, finish = exchange(result, send_two, recv_two, ssem_two, rsem_two)
    each_peer(start)
    recv_two[me] = send_two[me]
    each_peer(finish)
    coef_ref[...] = recv_two[...].reshape(rows, field_count)


def inverse_kernel(coef_ref, table_ref, out_ref):
    out_ref[0] = dot(coef_ref[...], table_ref[...], TN).astype(BF16)


def per_device(
    groups,
    grid_in,
    legendre,
    gauss_weight,
    vertical_modes,
    coupling,
    mode_rates,
    loop_length,
    lat_order,
    wave_number,
):
    loop_count, field_count, width = grid_in.shape
    assert loop_count == 1 and legendre.shape[0] == 1
    rows = 2 * groups
    levels = vertical_modes.shape[0]
    kpad = -(-levels // 128) * 128
    chunks = chunk_bounds(width // 128, 8)
    vmem = pl.BlockSpec(memory_space=pltpu.VMEM)
    flipped = jnp.swapaxes(legendre, 2, 3)
    slot = pltpu.VMEM((groups, 2, field_count), BF16)
    sems = pltpu.SemaphoreType.DMA((groups,))
    coef, table = pl.pallas_call(
        functools.partial(main_kernel, groups, chunks),
        out_shape=(
            jax.ShapeDtypeStruct((rows, field_count), BF16),
            jax.ShapeDtypeStruct((rows, width), BF16),
        ),
        in_specs=[pl.BlockSpec(memory_space=pltpu.HBM)] * 9,
        out_specs=(vmem, vmem),
        scratch_shapes=[
            pltpu.VMEM((field_count, width), BF16),
            pltpu.VMEM(flipped.shape, BF16),
            pltpu.SMEM(gauss_weight.shape, F32),
            pltpu.VMEM(vertical_modes.shape, F32),
            pltpu.VMEM(coupling.shape, F32),
            pltpu.VMEM(mode_rates.shape, F32),
            pltpu.SMEM(loop_length.shape, jnp.int32),
            pltpu.SMEM(lat_order.shape, jnp.int32),
            pltpu.SMEM(wave_number.shape, jnp.int32),
            pltpu.VMEM((2 * levels, 2 * kpad), F32),
            pltpu.VMEM((2 * levels, kpad), F32),
            pltpu.VMEM((1, kpad), F32),
            slot,
            slot,
            slot,
            slot,
            pltpu.SemaphoreType.DMA((len(chunks),)),
            pltpu.SemaphoreType.DMA((8,)),
            sems,
            sems,
            sems,
            sems,
        ],
        compiler_params=pltpu.CompilerParams(
            collective_id=0, has_side_effects=True, vmem_limit_bytes=32 * 1024 * 1024
        ),
        name="forward_spectral",
    )(
        *[
            pltpu.with_memory_space_constraint(x, pltpu.HBM)
            for x in (
                grid_in,
                flipped,
                gauss_weight,
                vertical_modes,
                coupling,
                mode_rates,
                loop_length,
                lat_order,
                wave_number,
            )
        ]
    )
    tile = 640
    return pl.pallas_call(
        inverse_kernel,
        grid=(-(-width // tile),),
        out_shape=jax.ShapeDtypeStruct(grid_in.shape, BF16),
        in_specs=[
            pl.BlockSpec((rows, field_count), lambda i: (0, 0)),
            pl.BlockSpec((rows, tile), lambda i: (0, i)),
        ],
        out_specs=pl.BlockSpec((1, field_count, tile), lambda i: (0, 0, i)),
        compiler_params=pltpu.CompilerParams(vmem_limit_bytes=32 * 1024 * 1024),
        name="inverse",
    )(coef, table)


def solution(mesh):
    groups = mesh.shape["band"]
    placed = (
        P(("member", "band"), None, None),
        P("band", None, None, None),
        P(),
        P(),
        P(),
        P(),
        P(),
        P(),
        P(),
    )
    return jax.shard_map(
        functools.partial(per_device, groups),
        mesh=mesh,
        in_specs=placed,
        out_specs=P(("member", "band"), None, None),
        check_vma=False,
    )
```

```python
import functools
import math

import jax
import jax.numpy as jnp
from jax import lax
from jax.experimental import pallas as pl
from jax.experimental.pallas import tpu as pltpu
from jax.sharding import PartitionSpec as P

TRUNC = 1279
STEP = 0.5
F32 = jnp.float32
BF16 = jnp.bfloat16
HIGHEST = lax.Precision.HIGHEST
NT = (((1,), (1,)), ((), ()))
NN = (((1,), (0,)), ((), ()))
TN = (((0,), (0,)), ((), ()))


def dot(a, b, dims=NN, precision=None):
    return lax.dot_general(a, b, dims, precision=precision, preferred_element_type=F32)


def iota(shape, dim):
    return lax.broadcasted_iota(jnp.int32, shape, dim)


def sin_cos(turns, quarter_shift):
    quarter = jnp.floor(4.0 * turns + 0.5)
    y = (turns - 0.25 * quarter) * (2.0 * math.pi)
    z = y * y
    sine = y + y * z * (-1.6666654611e-1 + z * (8.3321608736e-3 + z * (-1.9515295891e-4)))
    cosine = 1.0 - 0.5 * z + z * z * (4.166664568298827e-2 + z * (-1.388731625493765e-3 + z * 2.443315711809948e-5))
    k = quarter.astype(jnp.int32) - quarter_shift
    swap = (k & 1) == 1
    cos_sign = jnp.where(((k + 1) & 2) == 0, 1.0, -1.0)
    sin_sign = jnp.where((k & 2) == 0, 1.0, -1.0)
    return (
        cos_sign * jnp.where(swap, sine, cosine),
        sin_sign * jnp.where(swap, cosine, sine),
    )


def spread(values, index, start):
    out = jnp.full(index.shape, start, F32)
    for at, value in enumerate(values):
        out = jnp.where(index == at, value, out)
    return out


def chunk_bounds(blocks, pieces):
    edges = [blocks * i // pieces for i in range(pieces + 1)]
    return [(a * 128, b * 128) for a, b in zip(edges[:-1], edges[1:]) if b > a]


def main_kernel(
    groups,
    chunks,
    grid_hbm,
    leg_hbm,
    gauss_hbm,
    modes_hbm,
    coupling_hbm,
    rates_hbm,
    length_hbm,
    order_hbm,
    wave_hbm,
    coef_ref,
    table_ref,
    grid_vmem,
    leg_ref,
    gauss_ref,
    modes_ref,
    coupling_ref,
    rates_ref,
    length_ref,
    order_ref,
    wave_ref,
    wf_ref,
    wb_ref,
    mu_ref,
    send_one,
    recv_one,
    send_two,
    recv_two,
    in_sem,
    small_sem,
    ssem_one,
    rsem_one,
    ssem_two,
    rsem_two,
):
    me = lax.axis_index("band")
    field_count, width = grid_vmem.shape
    levels = modes_ref.shape[0]
    nh, half_rows = leg_ref.shape[2], leg_ref.shape[3]
    lats = order_ref.shape[0]
    rows = 2 * groups
    kpad = wb_ref.shape[1]

    scalars = []
    smalls = []
    for at, (source, target) in enumerate(
        (
            (order_hbm, order_ref),
            (length_hbm, length_ref),
            (wave_hbm, wave_ref),
            (gauss_hbm, gauss_ref),
            (leg_hbm, leg_ref),
            (modes_hbm, modes_ref),
            (coupling_hbm, coupling_ref),
            (rates_hbm, rates_ref),
        )
    ):
        copy = pltpu.make_async_copy(source, target, small_sem.at[at])
        copy.start()
        (scalars if at < 4 else smalls).append(copy)
    loads = []
    for at, (lo, hi) in enumerate(chunks):
        copy = pltpu.make_async_copy(
            grid_hbm.at[0, :, lo:hi], grid_vmem.at[:, lo:hi], in_sem.at[at]
        )
        copy.start()
        loads.append(copy)

    barrier = pltpu.get_barrier_semaphore()

    def each_peer(body):
        if groups <= 16:
            for step in sorted(range(1, groups), key=lambda k: abs(2 * k - groups)):
                body(lax.rem(me + step, groups))
        else:

            def step_body(step, carry):
                body(lax.rem(me + step, groups))
                return carry

            lax.fori_loop(1, groups, step_body, 0)

    each_peer(lambda peer: pl.semaphore_signal(barrier, inc=1, device_id={"band": peer}))

    for copy in scalars:
        copy.wait()

    length = length_ref[order_ref[me]]
    length_f = length.astype(F32)
    row_id = iota((rows, 128), 0)
    lane_id = iota((rows, 128), 1)
    row_q = row_id & 1
    wave_rows = spread([wave_ref[d].astype(F32) for d in range(groups)], row_id >> 1, 0.0)
    inverse_len = 1.0 / jnp.full((rows, 128), length_f, F32)

    def turns_of(product):
        return (product - jnp.floor(product * inverse_len + 0.5) * length_f) * inverse_len

    inner_c, inner_s = sin_cos(turns_of(wave_rows * lane_id.astype(F32)), row_q)
    outer_c, outer_s = sin_cos(turns_of(wave_rows * (lane_id * 128).astype(F32)), 0)
    scale = jnp.where(2.0 * wave_rows < length_f, inverse_len, 0.0)
    scale = jnp.where(row_q == 0, scale, -scale)[:, :1]
    for a in range(width // 128):
        block = outer_c[:, a : a + 1] * inner_c - outer_s[:, a : a + 1] * inner_s
        block = jnp.where(lane_id < length - 128 * a, block, 0.0)
        table_ref[:, a * 128 : (a + 1) * 128] = block.astype(BF16)

    total = jnp.zeros((rows, field_count), F32)
    for copy, (lo, hi) in zip(loads, chunks):
        copy.wait()
        total += dot(table_ref[:, lo:hi], grid_vmem[:, lo:hi], NT)
    fourier = total * scale

    def exchange(values, send, recv, ssem, rsem):
        packed = values.astype(BF16)
        for d in range(groups):
            send[d] = packed[2 * d : 2 * d + 2, :]

        def start(peer):
            pltpu.make_async_remote_copy(
                src_ref=send.at[peer],
                dst_ref=recv.at[me],
                send_sem=ssem,
                recv_sem=rsem,
                device_id={"band": peer},
            ).start()

        others = pltpu.make_async_remote_copy(
            src_ref=send.at[0 : groups - 1],
            dst_ref=recv.at[0 : groups - 1],
            send_sem=ssem,
            recv_sem=rsem,
            device_id={"band": lax.rem(me + 1, groups)},
        )
        each_peer(start)
        recv[me] = send[me]
        return others

    pl.semaphore_wait(barrier, groups - 1)
    first = exchange(fourier, send_one, recv_one, ssem_one, rsem_one)

    for copy in smalls:
        copy.wait()
    modes = modes_ref[...]
    coupling = coupling_ref[...]
    wf_ref[...] = jnp.zeros(wf_ref.shape, F32)
    wb_ref[...] = jnp.zeros(wb_ref.shape, F32)
    mu_ref[...] = jnp.zeros(mu_ref.shape, F32)
    mu_ref[:, 0:levels] = rates_ref[...].reshape(1, levels)
    wf_ref[0:levels, 0:levels] = modes
    wf_ref[levels : 2 * levels, kpad : kpad + levels] = dot(coupling, modes, TN, HIGHEST)
    wb_ref[0:levels, 0:levels] = modes
    wb_ref[levels : 2 * levels, 0:levels] = -STEP * dot(coupling, modes, NN, HIGHEST)
    wf = wf_ref[...].astype(BF16)
    wb = wb_ref[...].astype(BF16)

    wave = wave_ref[me]
    order = [order_ref[i] for i in range(lats)]
    order_f = [o.astype(F32) for o in order]
    gauss = [gauss_ref[jnp.minimum(o, lats - 1 - o)] for o in order]
    solved = [jnp.where(2 * wave < length_ref[o], 1.0, 0.0) for o in order]
    boost = jnp.where(wave == 0, 1.0, 2.0)

    lane_one = iota((1, 2 * rows), 1)
    lane_row = jnp.where(lane_one < rows, lane_one, lane_one - rows)
    lane_lat = spread(order_f, lane_row >> 1, 0.0)
    lane_gauss = spread(gauss, lane_row >> 1, 0.0)
    north_j = iota((nh, 2 * rows), 0).astype(F32)
    col_row = iota((rows, nh), 0)
    col_lat = spread(order_f, col_row >> 1, 0.0)
    col_scale = spread(solved, iota((rows, 1), 0) >> 1, 0.0) * boost
    col_scale = jnp.where((iota((rows, 1), 0) & 1) == 0, col_scale, -col_scale)
    col_j = iota((rows, nh), 1).astype(F32)

    denom = float(TRUNC * (TRUNC + 1))
    m_parts, lt_parts, g_parts = [], [], []
    for p in range(2):
        leg = leg_ref[0, p]
        degree = wave + p + 2 * iota((half_rows, 1), 0)
        damp = (degree * (degree + 1)).astype(F32) * (STEP / denom)
        degree_lane = wave + p + 2 * iota((1, half_rows), 1)
        kept = jnp.where(degree_lane <= TRUNC, 1.0, 0.0)
        g_parts.append(1.0 / (1.0 + damp * mu_ref[...]))
        sign = 1.0 if p == 0 else -1.0
        pick_lane = jnp.where(lane_lat == north_j, 1.0, 0.0) + jnp.where(
            lane_lat == (lats - 1) - north_j, sign, 0.0
        )
        pick_col = jnp.where(col_lat == col_j, 1.0, 0.0) + jnp.where(
            col_lat == (lats - 1) - col_j, sign, 0.0
        )
        weight = jnp.where(lane_one < rows, 1.0, -damp) * lane_gauss
        for q in range(2):
            chosen = jnp.where((lane_one & 1) == q, pick_lane, 0.0).astype(BF16)
            m_parts.append((dot(leg, chosen, TN) * weight).astype(BF16))
            chosen = jnp.where((col_row & 1) == q, pick_col, 0.0).astype(BF16)
            lt_parts.append((dot(chosen, leg) * kept * col_scale).astype(BF16))
    through = sum(dot(lt, m) for lt, m in zip(lt_parts, m_parts))[:, 0:rows].astype(BF16)

    first.wait_recv()
    arrived = recv_one[...].reshape(rows, field_count)
    in_modes = dot(arrived, wf).astype(BF16)
    stacked = jnp.concatenate([in_modes[:, :kpad], in_modes[:, kpad:]], axis=0)
    passed = dot(through, arrived)
    back = jnp.zeros((rows, kpad), F32)
    for at in range(4):
        solved_part = (dot(m_parts[at], stacked) * g_parts[at // 2]).astype(BF16)
        back += dot(lt_parts[at], solved_part)
    result = dot(back.astype(BF16), wb, NT)
    result += jnp.where(iota((rows, field_count), 1) >= levels, passed, 0.0)

    second = exchange(result, send_two, recv_two, ssem_two, rsem_two)
    first.wait_send()
    second.wait_recv()
    second.wait_send()
    coef_ref[...] = recv_two[...].reshape(rows, field_count)


def inverse_kernel(chunks, coef_ref, table_ref, out_hbm, points, sem):
    coef = coef_ref[...].astype(F32).T.astype(BF16)
    stores = []
    for at, (lo, hi) in enumerate(chunks):
        points[:, lo:hi] = dot(coef, table_ref[:, lo:hi]).astype(BF16)
        copy = pltpu.make_async_copy(points.at[:, lo:hi], out_hbm.at[0, :, lo:hi], sem.at[at])
        copy.start()
        stores.append(copy)
    for copy in stores:
        copy.wait()


def per_device(
    groups,
    grid_in,
    legendre,
    gauss_weight,
    vertical_modes,
    coupling,
    mode_rates,
    loop_length,
    lat_order,
    wave_number,
):
    loop_count, field_count, width = grid_in.shape
    assert loop_count == 1 and legendre.shape[0] == 1
    rows = 2 * groups
    levels = vertical_modes.shape[0]
    kpad = -(-levels // 128) * 128
    chunks = chunk_bounds(width // 128, 8)
    stores = chunk_bounds(width // 128, 10)
    vmem = pl.BlockSpec(memory_space=pltpu.VMEM)
    flipped = jnp.swapaxes(legendre, 2, 3)
    slot = pltpu.VMEM((groups, 2, field_count), BF16)
    coef, table = pl.pallas_call(
        functools.partial(main_kernel, groups, chunks),
        out_shape=(
            jax.ShapeDtypeStruct((rows, field_count), BF16),
            jax.ShapeDtypeStruct((rows, width), BF16),
        ),
        in_specs=[pl.BlockSpec(memory_space=pltpu.HBM)] * 9,
        out_specs=(vmem, vmem),
        scratch_shapes=[
            pltpu.VMEM((field_count, width), BF16),
            pltpu.VMEM(flipped.shape, BF16),
            pltpu.SMEM(gauss_weight.shape, F32),
            pltpu.VMEM(vertical_modes.shape, F32),
            pltpu.VMEM(coupling.shape, F32),
            pltpu.VMEM(mode_rates.shape, F32),
            pltpu.SMEM(loop_length.shape, jnp.int32),
            pltpu.SMEM(lat_order.shape, jnp.int32),
            pltpu.SMEM(wave_number.shape, jnp.int32),
            pltpu.VMEM((2 * levels, 2 * kpad), F32),
            pltpu.VMEM((2 * levels, kpad), F32),
            pltpu.VMEM((1, kpad), F32),
            slot,
            slot,
            slot,
            slot,
            pltpu.SemaphoreType.DMA((len(chunks),)),
            pltpu.SemaphoreType.DMA((8,)),
            pltpu.SemaphoreType.DMA(()),
            pltpu.SemaphoreType.DMA(()),
            pltpu.SemaphoreType.DMA(()),
            pltpu.SemaphoreType.DMA(()),
        ],
        compiler_params=pltpu.CompilerParams(
            collective_id=0, has_side_effects=True, vmem_limit_bytes=32 * 1024 * 1024
        ),
        name="forward_spectral",
    )(
        *[
            pltpu.with_memory_space_constraint(x, pltpu.HBM)
            for x in (
                grid_in,
                flipped,
                gauss_weight,
                vertical_modes,
                coupling,
                mode_rates,
                loop_length,
                lat_order,
                wave_number,
            )
        ]
    )
    return pl.pallas_call(
        functools.partial(inverse_kernel, stores),
        out_shape=jax.ShapeDtypeStruct(grid_in.shape, BF16),
        in_specs=[vmem, vmem],
        out_specs=pl.BlockSpec(memory_space=pltpu.HBM),
        scratch_shapes=[
            pltpu.VMEM((field_count, width), BF16),
            pltpu.SemaphoreType.DMA((len(stores),)),
        ],
        compiler_params=pltpu.CompilerParams(vmem_limit_bytes=32 * 1024 * 1024),
        name="inverse",
    )(coef, table)


def solution(mesh):
    groups = mesh.shape["band"]
    placed = (
        P(("member", "band"), None, None),
        P("band", None, None, None),
        P(),
        P(),
        P(),
        P(),
        P(),
        P(),
        P(),
    )
    return jax.shard_map(
        functools.partial(per_device, groups),
        mesh=mesh,
        in_specs=placed,
        out_specs=P(("member", "band"), None, None),
        check_vma=False,
    )
```
